32 devices in a mesh: dp: 8 (over y, x, core), tensor: 4 (over z).
Axes of the slice: x: 2, y: 2, z: 4, core: 2. Of those that a mesh axis runs over, the one named last changes fastest.
Arguments:
- tokens: bfloat16 [512, 8192], P('dp'), may hold values from -6 to 6
- gate_weight: bfloat16 [8192, 14848], P('dp', 'tensor'), may hold values from -0.09375 to 0.09375
- up_weight: bfloat16 [8192, 14848], P('dp', 'tensor'), may hold values from -0.09375 to 0.09375
- down_weight: bfloat16 [14848, 8192], P('tensor', 'dp'), may hold values from -6 to 6
- channel_group: int32 [14848], P('tensor'), may hold values from 0 to 115, as said below
- owners: int32 [116], replicated, may hold values from 0 to 3
Outputs:
- group_scores: float32 [4, 116], P('tensor')
The draws below stay inside these ranges and needn't reach their ends.
Inputs may be any that keep to these rules, and one draw needn't show every extreme that they name: `channel_group`: every group 0 to 115 has exactly 128 channels.
All inputs are finite; a program needn't handle non-finite values.
Results may differ from the reference program's by a relative error of at most 0.0044.
Values may be sent and summed in bfloat16 or wider, within the bound.
A program may use at most 128 MiB of HBM per device.

```python
import jax
import jax.numpy as jnp
from jax import lax

D = 8192
FF = 14848
GROUP = 128
TOKENS = 512
GROUPS = 116
N_DP = 8
N_TENSOR = 4


def draw_channel_group(key, part):
    order = jax.random.permutation(jax.random.fold_in(key, 7), FF)
    return (order // GROUP).astype(jnp.int32)


def with_ends(result, own_key, low, high):
    extent = result.shape
    index_at = [jax.random.randint(jax.random.fold_in(own_key, axis), (), 0, extent[axis]) for axis in range(len(extent))]
    result = result.at[tuple(index_at)].set(low)
    longest = extent.index(max(extent))
    index_at[longest] = (index_at[longest] + 1) % extent[longest]
    return result.at[tuple(index_at)].set(high)


def spiked(drawn, own_key, source, target, blocks, factor):
    def block_of(position):
        return (jnp.arange(drawn.shape[position]) // (drawn.shape[position] // blocks)).reshape((-1,) + (1,) * (drawn.ndim - 1 - position))

    near = jax.random.permutation(own_key, blocks)[block_of(target)]
    second = (block_of(target) + blocks // 2) % blocks
    return jnp.where((block_of(source) == near) | (block_of(source) == second), factor * drawn, drawn)


def block_scale(stream_key, extent, shards, low, largest):
    level, own = 1.0, jax.random.fold_in(stream_key, 6)
    for position, blocks in shards:
        draws = jnp.exp(jax.random.uniform(jax.random.fold_in(own, position), (blocks,), jnp.float32, low / len(shards), largest / len(shards)))
        level = level * jnp.repeat(draws, extent[position] // blocks).reshape([-1 if axis == position else 1 for axis in range(len(extent))])
    return level


def noise(own_key, extent, spread, most, split=(), kind=jnp.bfloat16):
    result = jax.random.normal(own_key, extent, jnp.float32) * spread
    if len(split) > 0:
        result = block_scale(own_key, extent, split, -0.22, 0.18) * result
    return jnp.clip(result, min=-most, max=most).astype(kind)


def heavy_noise(stream_key, shape, spread, bound, cuts, heavy, held_as=jnp.bfloat16):
    entries = spread * jax.random.normal(stream_key, shape, jnp.float32)
    if cuts:
        entries = entries * block_scale(stream_key, shape, cuts, -0.22, 0.18)
    return jnp.clip(spiked(entries, jax.random.fold_in(stream_key, 3), *heavy), -bound, bound).astype(held_as)


def setup_inputs(seed: int = 0) -> dict:
    key_of = jax.random.split(jax.random.key(seed), 7)
    return {
        "tokens": noise(key_of[0], (TOKENS, D), 1.0, 6.0, ((0, 8),)),
        "gate_weight": heavy_noise(key_of[1], (D, FF), D ** -0.5, 0.09375, ((0, 8), (1, 4)), (0, 1, 8, 2.0)),
        "up_weight": heavy_noise(key_of[2], (D, FF), D ** -0.5, 0.09375, ((0, 8), (1, 4)), (0, 1, 8, 2.0)),
        "down_weight": heavy_noise(key_of[3], (FF, D), 1.0, 6.0, ((0, 4), (1, 8)), (1, 0, 8, 2.0)),
        "channel_group": draw_channel_group(jax.random.fold_in(key_of[6], 71), 0),
        "owners": with_ends(jax.random.randint(key_of[5], (GROUPS,), 0, N_TENSOR), jax.random.fold_in(key_of[5], 1), 0, N_TENSOR - 1).astype(jnp.int32),
    }


def reference(tokens, gate_weight, up_weight, down_weight, channel_group, owners):
    block = D // N_DP
    x_blocks = tokens.reshape(TOKENS, N_DP, block).transpose(1, 0, 2)
    g_blocks = gate_weight.reshape(N_DP, block, FF)
    u_blocks = up_weight.reshape(N_DP, block, FF)

    def add_block(carry, item):
        x_part, g_part, u_part = item
        pg = jnp.dot(x_part, g_part, preferred_element_type=jnp.float32).astype(jnp.bfloat16)
        pu = jnp.dot(x_part, u_part, preferred_element_type=jnp.float32).astype(jnp.bfloat16)
        pg, pu = lax.optimization_barrier((pg, pu))
        return ((carry[0] + pg.astype(jnp.float32), carry[1] + pu.astype(jnp.float32)), None)
    start = jnp.zeros((TOKENS, FF), jnp.float32)
    (gate, up), _ = lax.scan(add_block, (start, start), (x_blocks, g_blocks, u_blocks))
    hidden = jax.nn.silu(gate) * up
    energy = lax.optimization_barrier(jnp.sum(hidden * hidden, axis=0)) / TOKENS
    magnitude = lax.optimization_barrier(jnp.sum(jnp.abs(down_weight.astype(jnp.float32)), axis=1)) / D
    channel_score = jnp.sqrt(energy) * magnitude
    onehot = (channel_group[:, None] == jnp.arange(GROUPS, dtype=jnp.int32)[None, :]).astype(jnp.float32)
    totals = jnp.dot(channel_score, onehot, precision=lax.Precision.HIGHEST) / GROUP
    ranks = jnp.arange(N_TENSOR, dtype=jnp.int32)[:, None]
    return jnp.where(owners[None, :] == ranks, totals[None, :], jnp.float32(0.0))
```

```python
import functools

import jax
import jax.numpy as jnp
from jax import lax
from jax.experimental import pallas as pl
from jax.experimental.pallas import tpu as pltpu
from jax.sharding import PartitionSpec as P

GROUP = 128
LANES = 128
LAG_CORE = 2
LAG_FIRST = 5
LAG_SECOND = 8
MESH = pl.DeviceIdType.MESH


def group_sum(channel_score, groups, count):
    onehot = (groups[:, None] == jnp.arange(count, dtype=jnp.int32)[None, :]).astype(jnp.float32)
    return jnp.dot(channel_score, onehot, precision=lax.Precision.HIGHEST) / GROUP


def plain_shards(tokens, gate_weight, up_weight, down_weight, channel_group, owners):
    total_tokens = tokens.shape[0] * lax.axis_size("dp")
    width = gate_weight.shape[1]
    group_count = owners.shape[0]
    magnitude = jnp.sum(jnp.abs(down_weight.astype(jnp.float32)), axis=1) / tokens.shape[1]
    columns = lax.all_to_all(tokens, "dp", split_axis=1, concat_axis=0, tiled=True)
    mixed = lax.psum_scatter(
        jnp.concatenate(
            (
                jnp.dot(columns, gate_weight, preferred_element_type=jnp.float32),
                jnp.dot(columns, up_weight, preferred_element_type=jnp.float32),
            ),
            axis=1,
        ).astype(jnp.bfloat16),
        "dp",
        scatter_dimension=0,
        tiled=True,
    ).astype(jnp.float32)
    hidden = jax.nn.silu(mixed[:, :width]) * mixed[:, width:]
    energy = jnp.sum(hidden * hidden, axis=0) / total_tokens
    energy, magnitude = lax.psum((energy, magnitude), "dp")
    partial_value = group_sum(jnp.sqrt(energy) * magnitude, channel_group, group_count)
    totals = lax.psum(partial_value, "tensor")
    rank = lax.axis_index("tensor")
    row = jnp.where(owners == rank, totals, jnp.float32(0.0))
    return row[None, :]


def kernel(
    n_tensor,
    tok_ref,
    gate_ref,
    up_ref,
    down_ref,
    group_ref,
    owner_ref,
    out_ref,
    x_buf,
    w_buf,
    d_buf,
    part,
    got_core,
    got_first,
    got_second,
    energy,
    magnitude,
    score,
    totals,
    x_send,
    x_recv,
    local_sem,
    g_sem,
    u_sem,
    d_sem,
    core_send,
    core_recv,
    first_send,
    first_recv,
    second_send,
    second_recv,
    m_send,
    m_recv,
    e_send,
    e_recv,
    t_send,
    t_recv,
):
    n_dp = 8
    chunks = w_buf.shape[0]
    block = tok_ref.shape[0]
    depth = x_buf.shape[1]
    me = lax.axis_index("dp")
    z = lax.axis_index("tensor")
    c, x, y = me % 2, (me // 2) % 2, me // 4
    x_peer = me + 2 * (1 - 2 * x)
    y_peer = me + 4 * (1 - 2 * y)
    core_peer = me + (1 - 2 * c)
    first_peer = (1 - c) * x_peer + c * y_peer
    second_peer = (1 - c) * y_peer + c * x_peer

    def peer_of(k):
        bc, bx, by = k % 2, (k // 2) % 2, k // 4
        return me + bc * (1 - 2 * c) + 2 * bx * (1 - 2 * x) + 4 * by * (1 - 2 * y)

    def remote(src, dst, send, recv, peer):
        return pltpu.make_async_remote_copy(
            src_ref=src, dst_ref=dst, send_sem=send, recv_sem=recv, device_id=(peer, z), device_id_type=MESH
        )

    def gate_copy(i):
        cols = pl.ds(pl.multiple_of(i * LANES, LANES), LANES)
        return pltpu.make_async_copy(gate_ref.at[:, cols], w_buf.at[i, :, pl.ds(0, LANES)], g_sem.at[i])

    def up_copy(i):
        cols = pl.ds(pl.multiple_of(i * LANES, LANES), LANES)
        return pltpu.make_async_copy(up_ref.at[:, cols], w_buf.at[i, :, pl.ds(LANES, LANES)], u_sem.at[i])

    def down_copy(i):
        rows = pl.ds(pl.multiple_of(i * LANES, LANES), LANES)
        return pltpu.make_async_copy(down_ref.at[rows, :], d_buf.at[i], d_sem.at[i])

    barrier = pltpu.get_barrier_semaphore()
    for k in range(1, n_dp):
        pl.semaphore_signal(barrier, inc=1, device_id=(peer_of(k), z), device_id_type=MESH)
    for k in range(1, n_tensor):
        pl.semaphore_signal(barrier, inc=1, device_id=(me, (z + k) % n_tensor), device_id_type=MESH)

    own_cols = pl.ds(pl.multiple_of(me * depth, depth), depth)
    own_tokens = pltpu.make_async_copy(tok_ref.at[:, own_cols], x_buf.at[pl.ds(0, block), :], local_sem)
    own_tokens.start()

    @pl.loop(0, chunks)
    def _(i):
        down_copy(i).start()

    pl.semaphore_wait(barrier, n_dp - 1 + n_tensor - 1)

    token_copies = []
    for k in (6, 7, 2, 3, 4, 5, 1):
        bc, bx, by = k % 2, (k // 2) % 2, k // 4
        slot = bc * 4 + (1 - c) * (2 * bx + by) + c * (2 * by + bx)
        peer = peer_of(k)
        cols = pl.ds(pl.multiple_of(peer * depth, depth), depth)
        rows = pl.ds(pl.multiple_of(slot * block, block), block)
        copy = remote(tok_ref.at[:, cols], x_buf.at[rows, :], x_send.at[k - 1], x_recv.at[k - 1], peer)
        copy.start()
        token_copies.append(copy)

    @pl.loop(0, chunks)
    def _(i):
        gate_copy(i).start()
        up_copy(i).start()

    ones = jnp.ones((8, d_buf.shape[2]), jnp.bfloat16)

    @pl.loop(0, chunks)
    def _(i):
        down_copy(i).wait()
        sums = lax.dot_general(
            ones, jnp.abs(d_buf[i]), (((1,), (1,)), ((), ())), preferred_element_type=jnp.float32
        )
        magnitude[me, pl.ds(i, 1), :] = sums[0:1, :]

    own_tokens.wait()
    for copy in token_copies:
        copy.wait()

    m_copies = []
    for k in range(1, n_dp):
        copy = remote(magnitude.at[me], magnitude.at[me], m_send.at[k - 1], m_recv.at[k - 1], peer_of(k))
        copy.start()
        m_copies.append(copy)

    half, quarter, eighth = 4 * block, 2 * block, block

    def core_copy(i):
        return remote(
            part.at[i, pl.ds(half, half), :], got_core.at[i], core_send.at[i], core_recv.at[i], core_peer
        )

    def first_copy(i):
        return remote(
            part.at[i, pl.ds(quarter, quarter), :], got_first.at[i], first_send.at[i], first_recv.at[i], first_peer
        )

    def second_copy(i):
        return remote(
            part.at[i, pl.ds(eighth, eighth), :], got_second.at[i], second_send.at[i], second_recv.at[i], second_peer
        )

    def add(a, b):
        return (a.astype(jnp.float32) + b.astype(jnp.float32)).astype(jnp.bfloat16)

    def step(it, on):
        after_core, after_first, after_second = it - LAG_CORE, it - LAG_FIRST, it - LAG_SECOND

        @pl.when((after_core >= 0) & (after_core < chunks))
        def _():
            core_copy(after_core).wait_recv()
            part[after_core, :half, :] = add(part[after_core, :half, :], got_core[after_core])

        @pl.when((after_first >= 0) & (after_first < chunks))
        def _():
            first_copy(after_first).wait_recv()
            part[after_first, :quarter, :] = add(part[after_first, :quarter, :], got_first[after_first])

        @pl.when(it < chunks)
        def _():
            gate_copy(it).wait()
            up_copy(it).wait()
            part[it, half:, :] = jnp.dot(
                x_buf[half:, :], w_buf[it], preferred_element_type=jnp.float32
            ).astype(jnp.bfloat16)
            part[it, :half, :] = jnp.dot(
                x_buf[:half, :], w_buf[it], preferred_element_type=jnp.float32
            ).astype(jnp.bfloat16)

        @pl.when((after_first >= 0) & (after_first < chunks))
        def _():
            second_copy(after_first).start()

        @pl.when((after_core >= 0) & (after_core < chunks))
        def _():
            first_copy(after_core).start()

        @pl.when(it < chunks)
        def _():
            core_copy(it).start()

        @pl.when(after_second >= 0)
        def _():
            second_copy(after_second).wait_recv()
            mixed = part[after_second, :eighth, :].astype(jnp.float32) + got_second[after_second].astype(jnp.float32)
            gate, up = mixed[:, :LANES], mixed[:, LANES:]
            hidden = gate / (1.0 + jnp.exp(-gate)) * up
            energy[me, pl.ds(after_second, 1), :] = jnp.sum(hidden * hidden, axis=0, keepdims=True)

        return on

    lax.fori_loop(0, chunks + LAG_SECOND, step, 0)

    e_copies = []
    for k in range(1, n_dp):
        copy = remote(energy.at[me], energy.at[me], e_send.at[k - 1], e_recv.at[k - 1], peer_of(k))
        copy.start()
        e_copies.append(copy)
    for copy in m_copies:
        copy.wait()
    mag = magnitude[0]
    for r in range(1, n_dp):
        mag = mag + magnitude[r]
    mag = mag / tok_ref.shape[1]
    for copy in e_copies:
        copy.wait()
    total = energy[0]
    for r in range(1, n_dp):
        total = total + energy[r]
    score[...] = jnp.sqrt(total / (block * n_dp)) * mag

    lines = lax.broadcasted_iota(jnp.int32, (score_groups(owner_ref), LANES), 0)

    def gather(i, acc):
        hit = lines == group_ref[pl.ds(i, 1), :]
        return acc + jnp.where(hit, score[pl.ds(i, 1), :], 0.0)

    acc = lax.fori_loop(0, chunks, gather, jnp.zeros(lines.shape, jnp.float32))
    mine = jnp.sum(acc.T, axis=0, keepdims=True)
    totals[z] = jnp.broadcast_to(mine, totals.shape[1:])
    t_copies = []
    for k in range(1, n_tensor):
        copy = pltpu.make_async_remote_copy(
            src_ref=totals.at[z],
            dst_ref=totals.at[z],
            send_sem=t_send.at[k - 1],
            recv_sem=t_recv.at[k - 1],
            device_id=(me, (z + k) % n_tensor),
            device_id_type=MESH,
        )
        copy.start()
        t_copies.append(copy)

    @pl.loop(0, chunks)
    def _(i):
        core_copy(i).wait_send()
        first_copy(i).wait_send()
        second_copy(i).wait_send()

    for copy in t_copies:
        copy.wait()
    row = totals[0]
    for r in range(1, n_tensor):
        row = row + totals[r]
    row = row[0:1, : out_ref.shape[1]] / GROUP
    out_ref[...] = jnp.where(owner_ref[...] == z, row, 0.0)


def score_groups(owner_ref):
    return -(-owner_ref.shape[1] // LANES) * LANES


def fused_shards(n_dp, n_tensor, tokens, gate_weight, up_weight, down_weight, channel_group, owners):
    block = tokens.shape[0]
    depth, width = gate_weight.shape
    chunks = width // LANES
    count = owners.shape[0]
    span = down_weight.shape[1]
    rows = block * n_dp
    vmem = pl.BlockSpec(memory_space=pltpu.VMEM)
    hbm = pl.BlockSpec(memory_space=pl.ANY)
    padded = -(-count // LANES) * LANES
    dma = pltpu.SemaphoreType.DMA
    return pl.pallas_call(
        functools.partial(kernel, n_tensor),
        out_shape=jax.ShapeDtypeStruct((1, count), jnp.float32),
        in_specs=[hbm, hbm, hbm, hbm, vmem, vmem],
        out_specs=vmem,
        scratch_shapes=[
            pltpu.VMEM((rows, depth), jnp.bfloat16),
            pltpu.VMEM((chunks, depth, 2 * LANES), jnp.bfloat16),
            pltpu.VMEM((chunks, LANES, span), jnp.bfloat16),
            pltpu.VMEM((chunks, rows, 2 * LANES), jnp.bfloat16),
            pltpu.VMEM((chunks, rows // 2, 2 * LANES), jnp.bfloat16),
            pltpu.VMEM((chunks, rows // 4, 2 * LANES), jnp.bfloat16),
            pltpu.VMEM((chunks, rows // 8, 2 * LANES), jnp.bfloat16),
            pltpu.VMEM((n_dp, chunks, LANES), jnp.float32),
            pltpu.VMEM((n_dp, chunks, LANES), jnp.float32),
            pltpu.VMEM((chunks, LANES), jnp.float32),
            pltpu.VMEM((n_tensor, 8, padded), jnp.float32),
            dma((n_dp - 1,)),
            dma((n_dp - 1,)),
            dma,
            dma((chunks,)),
            dma((chunks,)),
            dma((chunks,)),
            dma((chunks,)),
            dma((chunks,)),
            dma((chunks,)),
            dma((chunks,)),
            dma((chunks,)),
            dma((chunks,)),
            dma((n_dp - 1,)),
            dma((n_dp - 1,)),
            dma((n_dp - 1,)),
            dma((n_dp - 1,)),
            dma((max(n_tensor - 1, 1),)),
            dma((max(n_tensor - 1, 1),)),
        ],
        compiler_params=pltpu.CompilerParams(
            collective_id=0, has_side_effects=True, vmem_limit_bytes=56 * 1024 * 1024
        ),
    )(tokens, gate_weight, up_weight, down_weight, channel_group.reshape(chunks, LANES), owners.reshape(1, count))


def solution(mesh):
    n_dp, n_tensor = mesh.shape["dp"], mesh.shape["tensor"]

    def shards(tokens, gate_weight, *rest):
        if n_dp == 8 and gate_weight.shape[1] % LANES == 0:
            return fused_shards(n_dp, n_tensor, tokens, gate_weight, *rest)
        return plain_shards(tokens, gate_weight, *rest)

    return jax.shard_map(
        shards,
        mesh=mesh,
        in_specs=(
            P("dp", None),
            P("dp", "tensor"),
            P("dp", "tensor"),
            P("tensor", "dp"),
            P("tensor"),
            P(),
        ),
        out_specs=P("tensor", None),
        check_vma=False,
    )
```

```python
import functools

import jax
import jax.numpy as jnp
from jax import lax
from jax.experimental import pallas as pl
from jax.experimental.pallas import tpu as pltpu
from jax.sharding import PartitionSpec as P

GROUP = 128
LANES = 128
LAG_CORE = 3
LAG_FIRST = 8
LAG_SECOND = 13
MESH = pl.DeviceIdType.MESH


def group_sum(channel_score, groups, count):
    onehot = (groups[:, None] == jnp.arange(count, dtype=jnp.int32)[None, :]).astype(jnp.float32)
    return jnp.dot(channel_score, onehot, precision=lax.Precision.HIGHEST) / GROUP


def plain_shards(tokens, gate_weight, up_weight, down_weight, channel_group, owners):
    total_tokens = tokens.shape[0] * lax.axis_size("dp")
    width = gate_weight.shape[1]
    group_count = owners.shape[0]
    magnitude = jnp.sum(jnp.abs(down_weight.astype(jnp.float32)), axis=1) / tokens.shape[1]
    columns = lax.all_to_all(tokens, "dp", split_axis=1, concat_axis=0, tiled=True)
    mixed = lax.psum_scatter(
        jnp.concatenate(
            (
                jnp.dot(columns, gate_weight, preferred_element_type=jnp.float32),
                jnp.dot(columns, up_weight, preferred_element_type=jnp.float32),
            ),
            axis=1,
        ).astype(jnp.bfloat16),
        "dp",
        scatter_dimension=0,
        tiled=True,
    ).astype(jnp.float32)
    hidden = jax.nn.silu(mixed[:, :width]) * mixed[:, width:]
    energy = jnp.sum(hidden * hidden, axis=0) / total_tokens
    energy, magnitude = lax.psum((energy, magnitude), "dp")
    partial_value = group_sum(jnp.sqrt(energy) * magnitude, channel_group, group_count)
    totals = lax.psum(partial_value, "tensor")
    rank = lax.axis_index("tensor")
    row = jnp.where(owners == rank, totals, jnp.float32(0.0))
    return row[None, :]


def kernel(
    n_tensor,
    tok_ref,
    gate_ref,
    up_ref,
    down_ref,
    group_ref,
    owner_ref,
    out_ref,
    tok_buf,
    x_buf,
    w_buf,
    d_buf,
    part,
    got_core,
    got_first,
    got_second,
    energy,
    magnitude,
    score,
    totals,
    x_send,
    x_recv,
    local_sem,
    g_sem,
    u_sem,
    d_sem,
    core_send,
    core_recv,
    first_send,
    first_recv,
    second_send,
    second_recv,
    m_send,
    m_recv,
    early_send,
    early_recv,
    e_send,
    e_recv,
    t_send,
    t_recv,
):
    n_dp = 8
    chunks = w_buf.shape[0]
    block = tok_ref.shape[0]
    depth = x_buf.shape[1]
    me = lax.axis_index("dp")
    z = lax.axis_index("tensor")
    c, x, y = me % 2, (me // 2) % 2, me // 4
    x_peer = me + 2 * (1 - 2 * x)
    y_peer = me + 4 * (1 - 2 * y)
    core_peer = me + (1 - 2 * c)
    first_peer = (1 - c) * x_peer + c * y_peer
    second_peer = (1 - c) * y_peer + c * x_peer

    def peer_of(k):
        bc, bx, by = k % 2, (k // 2) % 2, k // 4
        return me + bc * (1 - 2 * c) + 2 * bx * (1 - 2 * x) + 4 * by * (1 - 2 * y)

    def remote(src, dst, send, recv, peer):
        return pltpu.make_async_remote_copy(
            src_ref=src, dst_ref=dst, send_sem=send, recv_sem=recv, device_id=(peer, z), device_id_type=MESH
        )

    def gate_copy(i):
        cols = pl.ds(pl.multiple_of(i * LANES, LANES), LANES)
        return pltpu.make_async_copy(gate_ref.at[:, cols], w_buf.at[i, :, pl.ds(0, LANES)], g_sem.at[i])

    def up_copy(i):
        cols = pl.ds(pl.multiple_of(i * LANES, LANES), LANES)
        return pltpu.make_async_copy(up_ref.at[:, cols], w_buf.at[i, :, pl.ds(LANES, LANES)], u_sem.at[i])

    def down_copy(i):
        rows = pl.ds(pl.multiple_of(i * LANES, LANES), LANES)
        return pltpu.make_async_copy(down_ref.at[rows, :], d_buf.at[i], d_sem.at[i])

    load_tokens = pltpu.make_async_copy(tok_ref, tok_buf, local_sem)
    load_tokens.start()
    barrier = pltpu.get_barrier_semaphore()
    for k in range(1, n_dp):
        pl.semaphore_signal(barrier, inc=1, device_id=(peer_of(k), z), device_id_type=MESH)
    for k in range(1, n_tensor):
        pl.semaphore_signal(barrier, inc=1, device_id=(me, (z + k) % n_tensor), device_id_type=MESH)

    own_cols = pl.ds(pl.multiple_of(me * depth, depth), depth)

    @pl.loop(0, chunks)
    def _(i):
        down_copy(i).start()

    load_tokens.wait()
    pl.semaphore_wait(barrier, n_dp - 1 + n_tensor - 1)

    token_copies = []
    for k in (6, 7, 2, 3, 4, 5, 1):
        bc, bx, by = k % 2, (k // 2) % 2, k // 4
        slot = bc * 4 + (1 - c) * (2 * bx + by) + c * (2 * by + bx)
        peer = peer_of(k)
        cols = pl.ds(pl.multiple_of(peer * depth, depth), depth)
        rows = pl.ds(pl.multiple_of(slot * block, block), block)
        copy = remote(tok_buf.at[:, cols], x_buf.at[rows, :], x_send.at[k - 1], x_recv.at[k - 1], peer)
        copy.start()
        token_copies.append(copy)

    @pl.loop(0, chunks)
    def _(i):
        gate_copy(i).start()
        up_copy(i).start()

    ones = jnp.ones((8, d_buf.shape[2]), jnp.bfloat16)

    @pl.loop(0, chunks)
    def _(i):
        down_copy(i).wait()
        sums = lax.dot_general(
            ones, jnp.abs(d_buf[i]), (((1,), (1,)), ((), ())), preferred_element_type=jnp.float32
        )
        magnitude[me, pl.ds(i, 1), :] = sums[0:1, :]

    x_buf[:block, :] = tok_buf[:, own_cols]
    for copy in token_copies:
        copy.wait()

    m_copies = []
    for k in range(1, n_dp):
        copy = remote(magnitude.at[me], magnitude.at[me], m_send.at[k - 1], m_recv.at[k - 1], peer_of(k))
        copy.start()
        m_copies.append(copy)

    early = (chunks - 1) // 8 * 8

    def early_copy(k):
        rows = energy.at[me, pl.ds(0, early), :]
        return remote(rows, rows, early_send.at[k - 1], early_recv.at[k - 1], peer_of(k))

    def late_copy(k):
        rows = energy.at[me, pl.ds(early, chunks - early), :]
        return remote(rows, rows, e_send.at[k - 1], e_recv.at[k - 1], peer_of(k))

    half, quarter, eighth = 4 * block, 2 * block, block

    def core_copy(i):
        return remote(
            part.at[i, pl.ds(half, half), :], got_core.at[i], core_send.at[i], core_recv.at[i], core_peer
        )

    def first_copy(i):
        return remote(
            part.at[i, pl.ds(quarter, quarter), :], got_first.at[i], first_send.at[i], first_recv.at[i], first_peer
        )

    def second_copy(i):
        return remote(
            part.at[i, pl.ds(eighth, eighth), :], got_second.at[i], second_send.at[i], second_recv.at[i], second_peer
        )

    def add(a, b):
        return (a.astype(jnp.float32) + b.astype(jnp.float32)).astype(jnp.bfloat16)

    def step(it, on):
        after_core, after_first, after_second = it - LAG_CORE, it - LAG_FIRST, it - LAG_SECOND

        @pl.when((after_core >= 0) & (after_core < chunks))
        def _():
            core_copy(after_core).wait_recv()
            part[after_core, :half, :] = add(part[after_core, :half, :], got_core[after_core])

        @pl.when((after_first >= 0) & (after_first < chunks))
        def _():
            first_copy(after_first).wait_recv()
            part[after_first, :quarter, :] = add(part[after_first, :quarter, :], got_first[after_first])

        @pl.when(it < chunks)
        def _():
            gate_copy(it).wait()
            up_copy(it).wait()
            part[it, half:, :] = jnp.dot(
                x_buf[half:, :], w_buf[it], preferred_element_type=jnp.float32
            ).astype(jnp.bfloat16)
            part[it, :half, :] = jnp.dot(
                x_buf[:half, :], w_buf[it], preferred_element_type=jnp.float32
            ).astype(jnp.bfloat16)

        @pl.when((after_first >= 0) & (after_first < chunks))
        def _():
            second_copy(after_first).start()

        @pl.when((after_core >= 0) & (after_core < chunks))
        def _():
            first_copy(after_core).start()

        @pl.when(it < chunks)
        def _():
            core_copy(it).start()

        @pl.when(after_second == early)
        def _():
            for k in range(1, n_dp):
                early_copy(k).start()

        @pl.when(after_second >= 0)
        def _():
            second_copy(after_second).wait_recv()
            mixed = part[after_second, :eighth, :].astype(jnp.float32) + got_second[after_second].astype(jnp.float32)
            gate, up = mixed[:, :LANES], mixed[:, LANES:]
            hidden = gate / (1.0 + jnp.exp(-gate)) * up
            energy[me, pl.ds(after_second, 1), :] = jnp.sum(hidden * hidden, axis=0, keepdims=True)

        return on

    lax.fori_loop(0, chunks + LAG_SECOND, step, 0)

    for k in range(1, n_dp):
        late_copy(k).start()
    for copy in m_copies:
        copy.wait()
    mag = magnitude[0]
    for r in range(1, n_dp):
        mag = mag + magnitude[r]
    mag = mag / tok_ref.shape[1]
    for k in range(1, n_dp):
        early_copy(k).wait()
        late_copy(k).wait_recv()
    total = energy[0]
    for r in range(1, n_dp):
        total = total + energy[r]
    score[...] = jnp.sqrt(total / (block * n_dp)) * mag

    lines = lax.broadcasted_iota(jnp.int32, (score_groups(owner_ref), LANES), 0)

    def gather(i, acc):
        hit = lines == group_ref[pl.ds(i, 1), :]
        return acc + jnp.where(hit, score[pl.ds(i, 1), :], 0.0)

    acc = lax.fori_loop(0, chunks, gather, jnp.zeros(lines.shape, jnp.float32))
    mine = jnp.sum(acc.T, axis=0, keepdims=True)
    totals[z] = jnp.broadcast_to(mine, totals.shape[1:])
    t_copies = []
    for k in range(1, n_tensor):
        copy = pltpu.make_async_remote_copy(
            src_ref=totals.at[z],
            dst_ref=totals.at[z],
            send_sem=t_send.at[k - 1],
            recv_sem=t_recv.at[k - 1],
            device_id=(me, (z + k) % n_tensor),
            device_id_type=MESH,
        )
        copy.start()
        t_copies.append(copy)

    for k in range(1, n_dp):
        late_copy(k).wait_send()

    @pl.loop(0, chunks)
    def _(i):
        core_copy(i).wait_send()
        first_copy(i).wait_send()
        second_copy(i).wait_send()

    for copy in t_copies:
        copy.wait()
    row = totals[0]
    for r in range(1, n_tensor):
        row = row + totals[r]
    row = row[0:1, : out_ref.shape[1]] / GROUP
    out_ref[...] = jnp.where(owner_ref[...] == z, row, 0.0)


def score_groups(owner_ref):
    return -(-owner_ref.shape[1] // LANES) * LANES


def fused_shards(n_dp, n_tensor, tokens, gate_weight, up_weight, down_weight, channel_group, owners):
    block = tokens.shape[0]
    depth, width = gate_weight.shape
    chunks = width // LANES
    count = owners.shape[0]
    span = down_weight.shape[1]
    rows = block * n_dp
    vmem = pl.BlockSpec(memory_space=pltpu.VMEM)
    hbm = pl.BlockSpec(memory_space=pl.ANY)
    padded = -(-count // LANES) * LANES
    dma = pltpu.SemaphoreType.DMA
    return pl.pallas_call(
        functools.partial(kernel, n_tensor),
        out_shape=jax.ShapeDtypeStruct((1, count), jnp.float32),
        in_specs=[hbm, hbm, hbm, hbm, vmem, vmem],
        out_specs=vmem,
        scratch_shapes=[
            pltpu.VMEM(tokens.shape, jnp.bfloat16),
            pltpu.VMEM((rows, depth), jnp.bfloat16),
            pltpu.VMEM((chunks, depth, 2 * LANES), jnp.bfloat16),
            pltpu.VMEM((chunks, LANES, span), jnp.bfloat16),
            pltpu.VMEM((chunks, rows, 2 * LANES), jnp.bfloat16),
            pltpu.VMEM((chunks, rows // 2, 2 * LANES), jnp.bfloat16),
            pltpu.VMEM((chunks, rows // 4, 2 * LANES), jnp.bfloat16),
            pltpu.VMEM((chunks, rows // 8, 2 * LANES), jnp.bfloat16),
            pltpu.VMEM((n_dp, chunks, LANES), jnp.float32),
            pltpu.VMEM((n_dp, chunks, LANES), jnp.float32),
            pltpu.VMEM((chunks, LANES), jnp.float32),
            pltpu.VMEM((n_tensor, 8, padded), jnp.float32),
            dma((n_dp - 1,)),
            dma((n_dp - 1,)),
            dma,
            dma((chunks,)),
            dma((chunks,)),
            dma((chunks,)),
            dma((chunks,)),
            dma((chunks,)),
            dma((chunks,)),
            dma((chunks,)),
            dma((chunks,)),
            dma((chunks,)),
            dma((n_dp - 1,)),
            dma((n_dp - 1,)),
            dma((n_dp - 1,)),
            dma((n_dp - 1,)),
            dma((n_dp - 1,)),
            dma((n_dp - 1,)),
            dma((max(n_tensor - 1, 1),)),
            dma((max(n_tensor - 1, 1),)),
        ],
        compiler_params=pltpu.CompilerParams(
            collective_id=0, has_side_effects=True, vmem_limit_bytes=56 * 1024 * 1024
        ),
    )(tokens, gate_weight, up_weight, down_weight, channel_group.reshape(chunks, LANES), owners.reshape(1, count))


def solution(mesh):
    n_dp, n_tensor = mesh.shape["dp"], mesh.shape["tensor"]

    def shards(tokens, gate_weight, *rest):
        if n_dp == 8 and gate_weight.shape[1] % LANES == 0:
            return fused_shards(n_dp, n_tensor, tokens, gate_weight, *rest)
        return plain_shards(tokens, gate_weight, *rest)

    return jax.shard_map(
        shards,
        mesh=mesh,
        in_specs=(
            P("dp", None),
            P("dp", "tensor"),
            P("dp", "tensor"),
            P("tensor", "dp"),
            P("tensor"),
            P(),
        ),
        out_specs=P("tensor", None),
        check_vma=False,
    )
```
